256 devices in a mesh: vox: 32 (over x, z), frm: 8 (over y, core).
Axes of the slice: x: 4, y: 4, z: 8, core: 2. Of those that a mesh axis runs over, the one named last changes fastest.
Arguments:
- casorati: float32 [256, 1048576], P('frm', 'vox'), may hold values from -6 to 6
- start_vectors: float32 [256, 64], replicated, may hold values from -6 to 6
Outputs:
- vectors: float32 [256, 64], replicated
- filtered: float32 [256, 1048576], P('frm', 'vox')
The draws below stay inside these ranges and needn't reach their ends.
All inputs are finite; a program needn't handle non-finite values.
Results may differ from the reference program's by a relative error of at most 0.0003.
Values sent between devices are 32-bit elements; how exact they have to be, the bound alone decides.
A program may use at most 64 MiB of HBM per device.

```python
import jax
import jax.numpy as jnp
from jax import lax

FRAMES = 256
VECS = 64
ITERS = 3
VOXELS = 1048576


def block_levels(key, extent, cuts, low, largest):
    factor_of = 1.0
    for axis_at, blocks in cuts:
        heights = jax.random.uniform(jax.random.fold_in(jax.random.fold_in(key, 6), axis_at), (blocks,), jnp.float32, low / len(cuts), largest / len(cuts))
        factor_of = factor_of * jnp.repeat(jnp.exp(heights), extent[axis_at] // blocks).reshape((-1,) + (1,) * (len(extent) - 1 - axis_at))
    return factor_of


def bell_draw(key, extent, scale, limit, split=(), kind=jnp.bfloat16):
    array = jax.random.normal(key, extent, jnp.float32) * scale
    if len(split) > 0:
        array = block_levels(key, extent, split, -0.22, 0.18) * array
    return jnp.clip(array, min=-limit, max=limit).astype(kind)


def setup_inputs(seed: int = 0) -> dict:
    splits = jax.random.split(jax.random.key(seed), 3)
    casorati = bell_draw(splits[0], (FRAMES, VOXELS), 1.0, 6.0, ((0, 8), (1, 32)), jnp.float32)
    start_vectors = bell_draw(splits[1], (FRAMES, VECS), 1.0, 6.0, (), jnp.float32)
    return dict(casorati=casorati, start_vectors=start_vectors)


def orthonormal(projected):
    small = jnp.dot(projected.T, projected, precision=lax.Precision.HIGHEST)
    lower = jnp.linalg.cholesky(small)
    return jax.scipy.linalg.solve_triangular(lower, projected.T, lower=True).T

def reference(casorati, start_vectors):
    high = lax.Precision.HIGHEST
    vectors = start_vectors
    for step in range(ITERS):
        image = jnp.dot(vectors.T, casorati, precision=high)
        projected = jnp.dot(casorati, image.T, precision=high)
        vectors = orthonormal(projected)
    image = jnp.dot(vectors.T, casorati, precision=high)
    filtered = casorati - jnp.dot(vectors, image, precision=high)
    return (vectors, filtered)
```

```python
import functools

import jax
import jax.numpy as jnp
from jax import lax
from jax.experimental import pallas as pl
from jax.experimental.pallas import tpu as pltpu
from jax.sharding import PartitionSpec as P

ITERS = 3
MESH = pl.DeviceIdType.MESH
HIGH = lax.Precision.HIGHEST
NY = 4
NX = 4
PARTS = 4
SUBS = 8


def orthonormal(projected):
    small = jnp.dot(projected.T, projected, precision=HIGH)
    lower = jnp.linalg.cholesky(small)
    return jax.scipy.linalg.solve_triangular(lower, projected.T, lower=True).T


def remote(src, dst, send, recv, axis, index):
    return pltpu.make_async_remote_copy(
        src_ref=src, dst_ref=dst, send_sem=send, recv_sem=recv,
        device_id={axis: index}, device_id_type=MESH,
    )


def cut(start, size):
    return pl.ds(pl.multiple_of(start, size), size)


def greet(peers):
    barrier = pltpu.get_barrier_semaphore()
    for axis, index in peers:
        pl.semaphore_signal(barrier, inc=1, device_id={axis: index}, device_id_type=MESH)
    pl.semaphore_wait(barrier, len(peers))


def gram_kernel(nf, nz, c_ref, gram_ref, keep_ref, cols, relay, part, rs, row, xb, zb, fin, full,
                local_sem, keep_sem, hop_send, hop_recv, near_send, near_recv, far_send, far_recv,
                mate_send, mate_recv, f_send, f_recv, x_send, x_recv, z_send, z_recv,
                ax_send, ax_recv, af_send, af_recv):
    me, vox = lax.axis_index("frm"), lax.axis_index("vox")
    y, core = lax.div(me, 2), lax.rem(me, 2)
    x, z = lax.div(vox, nz), lax.rem(vox, nz)
    rows, width = c_ref.shape[0], c_ref.shape[1] // nf
    half = width // 2
    piece = half // PARTS
    nb = (lax.rem(y + 1, NY), lax.rem(y + NY - 1, NY))
    back = (nb[1], nb[0])
    far = lax.rem(y + 2, NY)
    mate = y * 2 + 1 - core

    frm_peers = [("frm", lax.rem(me + r, nf)) for r in range(1, nf)]
    x_peers = [("vox", lax.rem(x + r, NX) * nz + z) for r in range(1, NX)]
    z_peers = [("vox", x * nz + lax.rem(z + r, nz)) for r in range(1, nz)]
    greet(frm_peers + x_peers + z_peers)

    mine = cut(me * rows, rows)
    sends = []
    hops = {}
    for c2 in range(2):
        for d in range(2):
            hops[d, c2] = remote(
                c_ref.at[:, pl.ds(pl.multiple_of((far * 2 + c2) * width + d * half, half), half)],
                relay.at[d, c2], hop_send.at[d, c2], hop_recv.at[d, c2], "frm", nb[d] * 2 + core)
            hops[d, c2].start()
            sends.append(hops[d, c2])
    for c2 in range(2):
        for d in range(2):
            copy = remote(
                c_ref.at[:, cut((nb[d] * 2 + c2) * width, width)], cols.at[mine, :],
                near_send.at[d, c2], near_recv.at[d, core], "frm", nb[d] * 2 + c2)
            copy.start()
            sends.append(copy)
    to_mate = remote(c_ref.at[:, cut(mate * width, width)], cols.at[mine, :], mate_send, mate_recv, "frm", mate)
    to_mate.start()
    sends.append(to_mate)
    local = pltpu.make_async_copy(c_ref.at[:, cut(me * width, width)], cols.at[mine, :], local_sem)
    local.start()

    for c2 in range(2):
        for d in range(2):
            hops[d, c2].wait_recv()
    for s in range(PARTS):
        for c2 in range(2):
            for d in range(2):
                origin = back[d] * 2 + core
                copy = remote(
                    relay.at[d, c2, :, pl.ds(s * piece, piece)],
                    cols.at[cut(origin * rows, rows), pl.ds(d * half + s * piece, piece)],
                    far_send.at[s, d, c2], far_recv.at[s, d, core], "frm", nb[d] * 2 + c2)
                copy.start()
                sends.append(copy)

    local.wait()
    from_mate = remote(
        c_ref.at[:, cut(mate * width, width)], cols.at[cut(mate * rows, rows), :], mate_send, mate_recv, "frm", mate)
    from_mate.wait_recv()
    for d in range(2):
        for c2 in range(2):
            origin = back[d] * 2 + c2
            remote(
                c_ref.at[:, cut(origin * width, width)], cols.at[cut(origin * rows, rows), :],
                near_send.at[d, c2], near_recv.at[d, c2], "frm", origin).wait_recv()

    part[...] = jnp.zeros_like(part)

    def gather(t, carry):
        s, d = lax.div(t, 2), lax.rem(t, 2)
        at = pl.multiple_of(d * half + s * piece, piece)
        for c2 in range(2):
            origin = far * 2 + c2
            remote(
                relay.at[d, c2, :, pl.ds(pl.multiple_of(s * piece, piece), piece)],
                cols.at[cut(origin * rows, rows), pl.ds(at, piece)],
                far_send.at[s, d, c2], far_recv.at[s, d, c2], "frm", origin).wait_recv()
        block = cols[:, pl.ds(at, piece)]
        part[...] += lax.dot_general(
            block, block, (((1,), (1,)), ((), ())), precision=HIGH, preferred_element_type=jnp.float32)
        return carry

    lax.fori_loop(0, 2 * PARTS, gather, 0)
    keep = pltpu.make_async_copy(cols, keep_ref, keep_sem)
    keep.start()

    copies = []
    for r in range(1, nf):
        peer = lax.rem(me + r, nf)
        copies.append(remote(part.at[cut(peer * rows, rows), :], rs.at[me], f_send.at[r], f_recv.at[r], "frm", peer))
        copies[-1].start()
    rs[me] = part[mine, :]
    for copy in copies:
        copy.wait_recv()
    sends += copies
    row[...] = functools.reduce(jnp.add, [rs[k] for k in range(nf)])

    eighth = rows // NX
    slot = cut(x * eighth, eighth)
    copies = []
    for r in range(1, NX):
        px = lax.rem(x + r, NX)
        copies.append(remote(
            row.at[cut(px * eighth, eighth), :], xb.at[x], x_send.at[r], x_recv.at[r], "vox", px * nz + z))
        copies[-1].start()
    xb[x] = row[slot, :]
    for copy in copies:
        copy.wait_recv()
    sends += copies
    zb[z] = functools.reduce(jnp.add, [xb[k] for k in range(NX)])

    copies = []
    for r in range(1, nz):
        copies.append(remote(
            zb.at[z], zb.at[z], z_send.at[r], z_recv.at[r], "vox", x * nz + lax.rem(z + r, nz)))
        copies[-1].start()
    for copy in copies:
        copy.wait_recv()
    sends += copies
    fin[slot, :] = functools.reduce(jnp.add, [zb[k] for k in range(nz)])

    copies = []
    for r in range(1, NX):
        copies.append(remote(
            fin.at[slot, :], fin.at[slot, :], ax_send.at[r], ax_recv.at[r], "vox", lax.rem(x + r, NX) * nz + z))
        copies[-1].start()
    for copy in copies:
        copy.wait_recv()
    sends += copies

    copies = []
    for r in range(1, nf):
        copies.append(remote(
            fin, full.at[mine, :], af_send.at[r], af_recv.at[r], "frm", lax.rem(me + r, nf)))
        copies[-1].start()
    for copy in sends:
        copy.wait_send()
    gram_ref[mine, :] = fin[...]
    for r in range(1, nf):
        peer = lax.rem(me + nf - r, nf)
        spot = cut(peer * rows, rows)
        remote(fin, full.at[spot, :], af_send.at[r], af_recv.at[r], "frm", peer).wait_recv()
        gram_ref[spot, :] = full[spot, :]
    for copy in copies:
        copy.wait_send()
    keep.wait()


def filter_kernel(nf, c_ref, keep_ref, vec_ref, vect_ref, out_ref, img, own, cols, res,
                  own_sem, cols_sem, out_sem, near_send, near_recv, far_send, far_recv,
                  m_send, m_recv):
    me = lax.axis_index("frm")
    y, core = lax.div(me, 2), lax.rem(me, 2)
    rows, width = c_ref.shape[0], c_ref.shape[1] // nf
    sub = width // SUBS
    nb = (lax.rem(y + 1, NY), lax.rem(y + NY - 1, NY))
    back = (nb[1], nb[0])
    far = lax.rem(y + 2, NY)
    mate = y * 2 + 1 - core
    load_cols = pltpu.make_async_copy(keep_ref, cols, cols_sem)
    load_cols.start()
    load_own = pltpu.make_async_copy(c_ref, own, own_sem)
    load_own.start()
    greet([("frm", nb[0] * 2 + core), ("frm", nb[1] * 2 + core), ("frm", mate)])

    chips = (y, back[0], back[1], far)

    def at(chip, side, s):
        return pl.ds(pl.multiple_of((chip * 2 + side) * width + s * sub, sub), sub)

    def near(d, s, chip):
        spot = img.at[:, at(chip, core, s)]
        return remote(spot, spot, near_send.at[d, s], near_recv.at[d, s], "frm", nb[d] * 2 + core)

    def relayed(d, s, chip):
        spot = img.at[:, at(chip, core, s)]
        return remote(spot, spot, far_send.at[s], far_recv.at[s], "frm", nb[d] * 2 + core)

    def across(which, s, side):
        spot = img.at[:, at(chips[which], side, s)]
        return remote(spot, spot, m_send.at[which, s], m_recv.at[which, s], "frm", mate)

    mine = vec_ref[cut(me * rows, rows), :]

    def clean(chip, side, s):
        spot = at(chip, side, s)
        res[:, spot] = own[:, spot] - jnp.dot(mine, img[:, spot], precision=HIGH, preferred_element_type=jnp.float32)
        pltpu.make_async_copy(res.at[:, spot], out_ref.at[:, spot], out_sem).start()

    load_cols.wait()

    def first(s, carry):
        img[:, at(y, core, s)] = jnp.dot(
            vect_ref[...], cols[:, cut(s * sub, sub)], precision=HIGH, preferred_element_type=jnp.float32)
        near(0, s, y).start()
        near(1, s, y).start()
        across(0, s, core).start()
        return carry

    lax.fori_loop(0, SUBS, first, 0)
    load_own.wait()

    def second(pair, carry):
        for odd in range(2):
            s = pair * 2 + odd
            for d in range(2):
                near(d, s, back[d]).wait_recv()
                across(1 + d, s, core).start()
                if d == odd:
                    relayed(d, s, back[d]).start()
            clean(y, core, s)
            clean(back[0], core, s)
            clean(back[1], core, s)
            for which in range(3):
                across(which, s, 1 - core).wait_recv()
                clean(chips[which], 1 - core, s)
        return carry

    lax.fori_loop(0, SUBS // 2, second, 0)

    def third(pair, carry):
        for odd in range(2):
            s = pair * 2 + odd
            relayed(odd, s, far).wait_recv()
            across(3, s, core).start()
            clean(far, core, s)
            across(3, s, 1 - core).wait_recv()
            clean(far, 1 - core, s)
        return carry

    lax.fori_loop(0, SUBS // 2, third, 0)

    def last(pair, carry):
        for odd in range(2):
            s = pair * 2 + odd
            for d in range(2):
                near(d, s, y).wait_send()
            relayed(odd, s, back[odd]).wait_send()
            for which in range(4):
                across(which, s, core).wait_send()
        return carry

    lax.fori_loop(0, SUBS // 2, last, 0)
    pltpu.make_async_copy(res, out_ref, out_sem).wait()


def body(nf, nz, casorati, start_vectors):
    rows, wide = casorati.shape
    frames = rows * nf
    width = wide // nf
    dma = pltpu.SemaphoreType.DMA
    f32 = jnp.float32
    vmem = pl.BlockSpec(memory_space=pltpu.VMEM)
    hbm = pl.BlockSpec(memory_space=pl.ANY)
    eighth = rows // NX
    gram, columns = pl.pallas_call(
        functools.partial(gram_kernel, nf, nz),
        name="gram",
        out_shape=(jax.ShapeDtypeStruct((frames, frames), f32), jax.ShapeDtypeStruct((frames, width), f32)),
        in_specs=[hbm],
        out_specs=(vmem, hbm),
        scratch_shapes=[
            pltpu.VMEM((frames, width), f32),
            pltpu.VMEM((2, 2, rows, width // 2), f32),
            pltpu.VMEM((frames, frames), f32),
            pltpu.VMEM((nf, rows, frames), f32),
            pltpu.VMEM((rows, frames), f32),
            pltpu.VMEM((NX, eighth, frames), f32),
            pltpu.VMEM((nz, eighth, frames), f32),
            pltpu.VMEM((rows, frames), f32),
            pltpu.VMEM((frames, frames), f32),
            dma, dma, dma((2, 2)), dma((2, 2)), dma((2, 2)), dma((2, 2)),
            dma((PARTS, 2, 2)), dma((PARTS, 2, 2)), dma, dma,
            dma((nf,)), dma((nf,)), dma((NX,)), dma((NX,)), dma((nz,)), dma((nz,)),
            dma((NX,)), dma((NX,)), dma((nf,)), dma((nf,)),
        ],
        compiler_params=pltpu.CompilerParams(collective_id=0, has_side_effects=True, vmem_limit_bytes=32 << 20),
    )(casorati)
    vectors = start_vectors
    for step in range(ITERS):
        vectors = orthonormal(jnp.dot(gram, vectors, precision=HIGH))
    filtered = pl.pallas_call(
        functools.partial(filter_kernel, nf),
        name="clean",
        out_shape=jax.ShapeDtypeStruct((rows, wide), f32),
        in_specs=[hbm, hbm, vmem, vmem],
        out_specs=hbm,
        scratch_shapes=[
            pltpu.VMEM((vectors.shape[1], wide), f32),
            pltpu.VMEM((rows, wide), f32),
            pltpu.VMEM((frames, width), f32),
            pltpu.VMEM((rows, wide), f32),
            dma, dma, dma, dma((2, SUBS)), dma((2, SUBS)), dma((SUBS,)), dma((SUBS,)),
            dma((4, SUBS)), dma((4, SUBS)),
        ],
        compiler_params=pltpu.CompilerParams(collective_id=1, has_side_effects=True, vmem_limit_bytes=40 << 20),
    )(casorati, columns, vectors, vectors.T)
    return (vectors, filtered)


def solution(mesh):
    nf, nz = mesh.shape["frm"], mesh.shape["vox"] // NX
    return jax.shard_map(
        functools.partial(body, nf, nz),
        mesh=mesh,
        in_specs=(P("frm", "vox"), P()),
        out_specs=(P(), P("frm", "vox")),
        check_vma=False,
    )
```

```python
import functools

import jax
import jax.numpy as jnp
from jax import lax
from jax.experimental import pallas as pl
from jax.experimental.pallas import tpu as pltpu
from jax.sharding import PartitionSpec as P

ITERS = 3
MESH = pl.DeviceIdType.MESH
HIGH = lax.Precision.HIGHEST
NY = 4
NX = 4
PARTS = 4
SUBS = 8


def orthonormal(vt, g_ref):
    count = vt.shape[0] // 8
    pt = jnp.dot(vt, g_ref[...], precision=HIGH, preferred_element_type=jnp.float32)
    twice = jnp.concatenate([pt, pt], axis=0)
    small = lax.dot_general(pt, twice, (((1,), (1,)), ((), ())), precision=HIGH, preferred_element_type=jnp.float32)
    lanes = 128
    wide = pt.shape[1] // lanes
    rows = [[small[8 * i:8 * i + 8, :]] + [pt[8 * i:8 * i + 8, lanes * q:lanes * (q + 1)] for q in range(wide)] for i in range(count)]
    line = lax.broadcasted_iota(jnp.int32, (8, lanes), 0)
    for k in range(count):
        spread = [[jnp.broadcast_to(rows[i][0][:, 8 * k + j:8 * k + j + 1], (8, lanes)) for j in range(8)] for i in range(k, count)]
        scale = jnp.zeros((8, lanes), jnp.float32)
        for j in range(8):
            root = lax.rsqrt(jnp.broadcast_to(spread[0][j][j:j + 1, :], (8, lanes)))
            scale = jnp.where(line == j, root, scale)
            low = [s[j] * root for s in spread]
            for t in range(j + 1, 8):
                factor = jnp.broadcast_to(low[0][t:t + 1, :], (8, lanes))
                for i in range(len(spread)):
                    spread[i][t] = spread[i][t] - low[i] * factor
            low[0] = jnp.where(line > j, low[0], 0.0)
            for q in range(wide + 1):
                pivot = jnp.broadcast_to(rows[k][q][j:j + 1, :], (8, lanes)) * root
                for i in range(len(spread)):
                    rows[k + i][q] = rows[k + i][q] - low[i] * pivot
        for q in range(1, wide + 1):
            rows[k][q] = rows[k][q] * scale
    return jnp.concatenate([jnp.concatenate(rows[i][1:], axis=1) for i in range(count)], axis=0)


def remote(src, dst, send, recv, axis, index):
    return pltpu.make_async_remote_copy(
        src_ref=src, dst_ref=dst, send_sem=send, recv_sem=recv,
        device_id={axis: index}, device_id_type=MESH,
    )


def cut(start, size):
    return pl.ds(pl.multiple_of(start, size), size)


def greet(peers):
    barrier = pltpu.get_barrier_semaphore()
    for axis, index in peers:
        pl.semaphore_signal(barrier, inc=1, device_id={axis: index}, device_id_type=MESH)
    pl.semaphore_wait(barrier, len(peers))


def kernel(nf, nz, c_ref, start_ref, vec_ref, out_ref, cols, relay, part, rs, row, xb, zb, fin, full, vmat, img, own, res,
           local_sem, own_sem, out_sem, hop_send, hop_recv, near_send, near_recv, far_send, far_recv,
           mate_send, mate_recv, f_send, f_recv, x_send, x_recv, z_send, z_recv,
           ax_send, ax_recv, af_send, af_recv, in_send, in_recv, if_send, if_recv, im_send, im_recv):
    me, vox = lax.axis_index("frm"), lax.axis_index("vox")
    y, core = lax.div(me, 2), lax.rem(me, 2)
    x, z = lax.div(vox, nz), lax.rem(vox, nz)
    rows, width = c_ref.shape[0], c_ref.shape[1] // nf
    half = width // 2
    piece = half // PARTS
    nb = (lax.rem(y + 1, NY), lax.rem(y + NY - 1, NY))
    back = (nb[1], nb[0])
    far = lax.rem(y + 2, NY)
    mate = y * 2 + 1 - core

    frm_peers = [("frm", lax.rem(me + r, nf)) for r in range(1, nf)]
    x_peers = [("vox", lax.rem(x + r, NX) * nz + z) for r in range(1, NX)]
    z_peers = [("vox", x * nz + lax.rem(z + r, nz)) for r in range(1, nz)]
    greet(frm_peers + x_peers + z_peers)

    mine = cut(me * rows, rows)
    sends = []
    hops = {}
    for c2 in range(2):
        for d in range(2):
            hops[d, c2] = remote(
                c_ref.at[:, pl.ds(pl.multiple_of((far * 2 + c2) * width + d * half, half), half)],
                relay.at[d, c2], hop_send.at[d, c2], hop_recv.at[d, c2], "frm", nb[d] * 2 + core)
            hops[d, c2].start()
            sends.append(hops[d, c2])
    for c2 in range(2):
        for d in range(2):
            copy = remote(
                c_ref.at[:, cut((nb[d] * 2 + c2) * width, width)], cols.at[mine, :],
                near_send.at[d, c2], near_recv.at[d, core], "frm", nb[d] * 2 + c2)
            copy.start()
            sends.append(copy)
    to_mate = remote(c_ref.at[:, cut(mate * width, width)], cols.at[mine, :], mate_send, mate_recv, "frm", mate)
    to_mate.start()
    sends.append(to_mate)
    local = pltpu.make_async_copy(c_ref.at[:, cut(me * width, width)], cols.at[mine, :], local_sem)
    local.start()
    load_own = pltpu.make_async_copy(c_ref, own, own_sem)
    load_own.start()

    for c2 in range(2):
        for d in range(2):
            hops[d, c2].wait_recv()
    for s in range(PARTS):
        for c2 in range(2):
            for d in range(2):
                origin = back[d] * 2 + core
                copy = remote(
                    relay.at[d, c2, :, pl.ds(s * piece, piece)],
                    cols.at[cut(origin * rows, rows), pl.ds(d * half + s * piece, piece)],
                    far_send.at[s, d, c2], far_recv.at[s, d, core], "frm", nb[d] * 2 + c2)
                copy.start()
                sends.append(copy)

    local.wait()
    from_mate = remote(
        c_ref.at[:, cut(mate * width, width)], cols.at[cut(mate * rows, rows), :], mate_send, mate_recv, "frm", mate)
    from_mate.wait_recv()
    for d in range(2):
        for c2 in range(2):
            origin = back[d] * 2 + c2
            remote(
                c_ref.at[:, cut(origin * width, width)], cols.at[cut(origin * rows, rows), :],
                near_send.at[d, c2], near_recv.at[d, c2], "frm", origin).wait_recv()

    part[...] = jnp.zeros_like(part)

    def gather(t, carry):
        s, d = lax.div(t, 2), lax.rem(t, 2)
        at = pl.multiple_of(d * half + s * piece, piece)
        for c2 in range(2):
            origin = far * 2 + c2
            remote(
                relay.at[d, c2, :, pl.ds(pl.multiple_of(s * piece, piece), piece)],
                cols.at[cut(origin * rows, rows), pl.ds(at, piece)],
                far_send.at[s, d, c2], far_recv.at[s, d, c2], "frm", origin).wait_recv()
        block = cols[:, pl.ds(at, piece)]
        part[...] += lax.dot_general(
            block, block, (((1,), (1,)), ((), ())), precision=HIGH, preferred_element_type=jnp.float32)
        return carry

    lax.fori_loop(0, 2 * PARTS, gather, 0)

    copies = []
    for r in range(1, nf):
        peer = lax.rem(me + r, nf)
        copies.append(remote(part.at[cut(peer * rows, rows), :], rs.at[me], f_send.at[r], f_recv.at[r], "frm", peer))
        copies[-1].start()
    rs[me] = part[mine, :]
    for copy in copies:
        copy.wait_recv()
    sends += copies
    row[...] = functools.reduce(jnp.add, [rs[k] for k in range(nf)])

    eighth = rows // NX
    slot = cut(x * eighth, eighth)
    copies = []
    for r in range(1, NX):
        px = lax.rem(x + r, NX)
        copies.append(remote(
            row.at[cut(px * eighth, eighth), :], xb.at[x], x_send.at[r], x_recv.at[r], "vox", px * nz + z))
        copies[-1].start()
    xb[x] = row[slot, :]
    for copy in copies:
        copy.wait_recv()
    sends += copies
    zb[z] = functools.reduce(jnp.add, [xb[k] for k in range(NX)])

    copies = []
    for r in range(1, nz):
        copies.append(remote(
            zb.at[z], zb.at[z], z_send.at[r], z_recv.at[r], "vox", x * nz + lax.rem(z + r, nz)))
        copies[-1].start()
    for copy in copies:
        copy.wait_recv()
    sends += copies
    fin[slot, :] = functools.reduce(jnp.add, [zb[k] for k in range(nz)])

    copies = []
    for r in range(1, NX):
        copies.append(remote(
            fin.at[slot, :], fin.at[slot, :], ax_send.at[r], ax_recv.at[r], "vox", lax.rem(x + r, NX) * nz + z))
        copies[-1].start()
    for copy in copies:
        copy.wait_recv()
    sends += copies

    copies = []
    for r in range(1, nf):
        copies.append(remote(
            fin, full.at[mine, :], af_send.at[r], af_recv.at[r], "frm", lax.rem(me + r, nf)))
        copies[-1].start()
    for copy in sends:
        copy.wait_send()
    full[mine, :] = fin[...]
    for r in range(1, nf):
        peer = lax.rem(me + nf - r, nf)
        spot = cut(peer * rows, rows)
        remote(fin, full.at[spot, :], af_send.at[r], af_recv.at[r], "frm", peer).wait_recv()
    for copy in copies:
        copy.wait_send()

    vec_ref[...] = start_ref[...]

    def turn(step, carry):
        vec_ref[...] = orthonormal(vec_ref[...], full)
        return carry

    lax.fori_loop(0, ITERS, turn, 0)
    vmat[...] = vec_ref[...].T

    sub = width // SUBS
    chips = (y, back[0], back[1], far)

    def at(chip, side, s):
        return pl.ds(pl.multiple_of((chip * 2 + side) * width + s * sub, sub), sub)

    def near(d, s, chip):
        spot = img.at[:, at(chip, core, s)]
        return remote(spot, spot, in_send.at[d, s], in_recv.at[d, s], "frm", nb[d] * 2 + core)

    def relayed(d, s, chip):
        spot = img.at[:, at(chip, core, s)]
        return remote(spot, spot, if_send.at[s], if_recv.at[s], "frm", nb[d] * 2 + core)

    def across(which, s, side):
        spot = img.at[:, at(chips[which], side, s)]
        return remote(spot, spot, im_send.at[which, s], im_recv.at[which, s], "frm", mate)

    basis = vmat[mine, :]

    def clean(chip, side, s):
        spot = at(chip, side, s)
        res[:, spot] = own[:, spot] - jnp.dot(basis, img[:, spot], precision=HIGH, preferred_element_type=jnp.float32)
        pltpu.make_async_copy(res.at[:, spot], out_ref.at[:, spot], out_sem).start()

    def first(s, carry):
        img[:, at(y, core, s)] = jnp.dot(
            vec_ref[...], cols[:, cut(s * sub, sub)], precision=HIGH, preferred_element_type=jnp.float32)
        near(0, s, y).start()
        near(1, s, y).start()
        across(0, s, core).start()
        return carry

    lax.fori_loop(0, SUBS, first, 0)
    load_own.wait()

    def second(pair, carry):
        for odd in range(2):
            s = pair * 2 + odd
            for d in range(2):
                near(d, s, back[d]).wait_recv()
                across(1 + d, s, core).start()
                if d == odd:
                    relayed(d, s, back[d]).start()
            clean(y, core, s)
            clean(back[0], core, s)
            clean(back[1], core, s)
            for which in range(3):
                across(which, s, 1 - core).wait_recv()
                clean(chips[which], 1 - core, s)
        return carry

    lax.fori_loop(0, SUBS // 2, second, 0)

    def third(pair, carry):
        for odd in range(2):
            s = pair * 2 + odd
            relayed(odd, s, far).wait_recv()
            across(3, s, core).start()
            clean(far, core, s)
            across(3, s, 1 - core).wait_recv()
            clean(far, 1 - core, s)
        return carry

    lax.fori_loop(0, SUBS // 2, third, 0)

    def last(pair, carry):
        for odd in range(2):
            s = pair * 2 + odd
            for d in range(2):
                near(d, s, y).wait_send()
            relayed(odd, s, back[odd]).wait_send()
            for which in range(4):
                across(which, s, core).wait_send()
        return carry

    lax.fori_loop(0, SUBS // 2, last, 0)
    pltpu.make_async_copy(res, out_ref, out_sem).wait()


def body(nf, nz, casorati, start_vectors):
    rows, wide = casorati.shape
    frames = rows * nf
    width = wide // nf
    dma = pltpu.SemaphoreType.DMA
    f32 = jnp.float32
    vmem = pl.BlockSpec(memory_space=pltpu.VMEM)
    hbm = pl.BlockSpec(memory_space=pltpu.HBM)
    eighth = rows // NX
    vecs = start_vectors.shape[1]
    vectors, filtered = pl.pallas_call(
        functools.partial(kernel, nf, nz),
        name="clutter",
        out_shape=(jax.ShapeDtypeStruct((vecs, frames), f32), jax.ShapeDtypeStruct((rows, wide), f32)),
        in_specs=[hbm, vmem],
        out_specs=(vmem, hbm),
        scratch_shapes=[
            pltpu.VMEM((frames, width), f32),
            pltpu.VMEM((2, 2, rows, width // 2), f32),
            pltpu.VMEM((frames, frames), f32),
            pltpu.VMEM((nf, rows, frames), f32),
            pltpu.VMEM((rows, frames), f32),
            pltpu.VMEM((NX, eighth, frames), f32),
            pltpu.VMEM((nz, eighth, frames), f32),
            pltpu.VMEM((rows, frames), f32),
            pltpu.VMEM((frames, frames), f32),
            pltpu.VMEM((frames, vecs), f32),
            pltpu.VMEM((vecs, wide), f32),
            pltpu.VMEM((rows, wide), f32),
            pltpu.VMEM((rows, wide), f32),
            dma, dma, dma, dma((2, 2)), dma((2, 2)), dma((2, 2)), dma((2, 2)),
            dma((PARTS, 2, 2)), dma((PARTS, 2, 2)), dma, dma,
            dma((nf,)), dma((nf,)), dma((NX,)), dma((NX,)), dma((nz,)), dma((nz,)),
            dma((NX,)), dma((NX,)), dma((nf,)), dma((nf,)),
            dma((2, SUBS)), dma((2, SUBS)), dma((SUBS,)), dma((SUBS,)), dma((4, SUBS)), dma((4, SUBS)),
        ],
        compiler_params=pltpu.CompilerParams(collective_id=0, has_side_effects=True, vmem_limit_bytes=56 << 20),
    )(casorati, start_vectors.T)
    return (vectors.T, filtered)


def solution(mesh):
    nf, nz = mesh.shape["frm"], mesh.shape["vox"] // NX
    return jax.shard_map(
        functools.partial(body, nf, nz),
        mesh=mesh,
        in_specs=(P("frm", "vox"), P()),
        out_specs=(P(), P("frm", "vox")),
        check_vma=False,
    )
```
